32 devices in a mesh: dp: 4 (over x, core), hist: 8 (over z, y).
Axes of the slice: x: 2, y: 2, z: 4, core: 2. Of those that a mesh axis runs over, the one named last changes fastest.
Arguments:
- candidates: bfloat16 [16, 512, 128], P('dp', 'hist'), may hold values from -150 to 150
- history: bfloat16 [16, 16384, 128], P('dp', 'hist'), may hold values from -6 to 6
- projections: bfloat16 [4, 128, 128], P(None, 'dp'), may hold values from -0.5 to 0.5
- lengths: int32 [16], P('dp'), may hold values from 8193 to 16384
- selected: int32 [16, 64], P('dp'), may hold values from 0 to 127, as said below
Outputs:
- interest: bfloat16 [16, 512, 128], P('dp', 'hist')
The draws below stay inside these ranges and needn't reach their ends.
Inputs may be any that keep to these rules, and one draw needn't show every extreme that they name: `selected`: each row names 64 different history blocks.
All inputs are finite; a program needn't handle non-finite values.
Results may differ from the reference program's by a relative error of at most 0.008.
The reference program's roundings to bfloat16 on the way count: a program that leaves them out, or rounds other values in their place, can miss the bound.
Values may be sent and summed in bfloat16 or wider, within the bound.
A program may use at most 128 MiB of HBM per device.

```python
import math
import jax
import jax.numpy as jnp
from jax import lax

D = 128
H = 4
HD = 32
CANDS = 512
BLOCK = 128
USERS = 16
HBLOCKS = 128
HIST = 16384
SEL = 64


def draw_candidates(key, part):
    base = jnp.clip(3.0 * jax.random.normal(key, (USERS, CANDS, D), jnp.float32), -18.0, 18.0)
    return base.astype(jnp.bfloat16)


def draw_history(key, part):
    base = jnp.clip(jax.random.normal(key, (USERS, HIST, D), jnp.float32), -6.0, 6.0)
    return base.astype(jnp.bfloat16)


def draw_selected(key, part):
    user_keys = jax.random.split(jax.random.fold_in(key, 3), USERS)
    orders = jax.vmap(lambda one_key: jax.random.permutation(one_key, HBLOCKS))(user_keys)
    return orders[:, :SEL].astype(jnp.int32)


def with_ends(entries, stream_key, smallest, high):
    index_at = [jax.random.randint(jax.random.fold_in(stream_key, axis), (), 0, length) for axis, length in enumerate(entries.shape)]
    longest = entries.shape.index(max(entries.shape))
    next_to = index_at[:longest] + [(index_at[longest] + 1) % entries.shape[longest]] + index_at[longest + 1:]
    return entries.at[tuple(index_at)].set(smallest).at[tuple(next_to)].set(high)


def level_of(own_key, dims, cuts, smallest, top_value):
    gain, own = 1.0, jax.random.fold_in(own_key, 6)
    for axis_at, blocks in cuts:
        steps = jnp.exp(jax.random.uniform(jax.random.fold_in(own, axis_at), (blocks,), jnp.float32, smallest / len(cuts), top_value / len(cuts)))
        gain = gain * jnp.repeat(steps, dims[axis_at] // blocks).reshape([-1 if axis == axis_at else 1 for axis in range(len(dims))])
    return gain


def gaussian(key, extent, deviation, bound, cuts=(), kind=jnp.bfloat16):
    drawn = jax.random.normal(key, extent, jnp.float32) * deviation
    if len(cuts) > 0:
        drawn = level_of(key, extent, cuts, -0.22, 0.18) * drawn
    return jnp.clip(drawn, min=-bound, max=bound).astype(kind)


def setup_inputs(seed: int = 0) -> dict:
    seeds = jax.random.split(jax.random.key(seed), 6)
    return {
        "candidates": draw_candidates(jax.random.fold_in(seeds[5], 71), 0),
        "history": draw_history(jax.random.fold_in(seeds[5], 71), 0),
        "projections": gaussian(seeds[2], (4, D, D), D ** -0.5, 0.5, ((1, 4),)),
        "lengths": with_ends(jax.random.randint(seeds[3], (USERS,), (HBLOCKS - SEL) * BLOCK + 1, HIST + 1), jax.random.fold_in(seeds[3], 1), (HBLOCKS - SEL) * BLOCK + 1, HIST).astype(jnp.int32),
        "selected": draw_selected(jax.random.fold_in(seeds[5], 71), 0),
    }


def reference(candidates, history, projections, lengths, selected):
    inv_root = 1.0 / math.sqrt(HD)
    offsets = jnp.arange(BLOCK, dtype=jnp.int32)

    def one_user(item):
        cand_rows, hist_rows, chosen, length = item
        queries = jnp.dot(cand_rows, projections[0], preferred_element_type=jnp.float32).astype(jnp.bfloat16)
        blocks = hist_rows.reshape(HBLOCKS, BLOCK, D)[chosen.astype(jnp.int32)].reshape(SEL * BLOCK, D)
        places = (chosen.astype(jnp.int32)[:, None] * BLOCK + offsets[None, :]).reshape(-1)
        live_keys = places < length
        keys = jnp.dot(blocks, projections[1], preferred_element_type=jnp.float32).astype(jnp.bfloat16)
        values = jnp.dot(blocks, projections[2], preferred_element_type=jnp.float32).astype(jnp.bfloat16)
        query_heads = queries.reshape(CANDS, H, HD).astype(jnp.float32)
        key_heads = keys.reshape(SEL * BLOCK, H, HD).astype(jnp.float32)
        value_heads = values.reshape(SEL * BLOCK, H, HD).astype(jnp.float32)
        scores = jnp.einsum('chd,khd->hck', query_heads, key_heads) * inv_root
        scores = jnp.where(live_keys[None, None, :], scores, -1e+30)
        maxima = lax.optimization_barrier(jnp.max(scores, axis=-1, keepdims=True))
        expo = jnp.where(live_keys[None, None, :], jnp.exp(scores - maxima), 0.0)
        totals = lax.optimization_barrier(jnp.sum(expo, axis=-1))
        rounded = lax.optimization_barrier(expo.astype(jnp.bfloat16)).astype(jnp.float32)
        summed = jnp.einsum('hck,khd->chd', rounded, value_heads)
        attended = (summed / totals.T[:, :, None]).reshape(CANDS, D).astype(jnp.bfloat16)
        return jnp.dot(attended, projections[3], preferred_element_type=jnp.float32).astype(jnp.bfloat16)
    return lax.map(one_user, (candidates, history, selected, lengths))
```

```python
import functools
import math

import jax
import jax.numpy as jnp
from jax import lax
from jax.experimental import pallas as pl
from jax.experimental.pallas import tpu as pltpu
from jax.sharding import PartitionSpec as P

H = 4
BLOCK = 128
PAIR = 2
LOW = -1e30


def attend_kernel(
    own_cands, lengths, selected, base, cand, hist, weights, parts, stats, qpad, acc, top, total, lse, live
):
    user = pl.program_id(0)
    users = pl.num_programs(0)
    cands, embed = cand.shape[1], cand.shape[2]
    head = embed // H
    factor = math.log2(math.e) / math.sqrt(head)
    blocks = hist.shape[1] // BLOCK
    length = lengths[user]
    first = base[0]
    chosen = selected.shape[1]

    def note(j, count):
        block = selected[user, j] - first
        live[count] = block
        ok = jnp.logical_and(block >= 0, block < blocks)
        ok = jnp.logical_and(ok, (block + first) * BLOCK < length)
        return count + jnp.where(ok, 1, 0)

    def note_many(j, count):
        for step in range(8):
            count = note(j * 8 + step, count)
        return count

    count = lax.fori_loop(0, chosen // 8, note_many, jnp.int32(0))

    query = lax.dot_general(
        weights[0], cand[0], (((0,), (1,)), ((), ())), preferred_element_type=jnp.float32
    ).astype(jnp.bfloat16)
    for h in range(H):
        rows = slice(h * head, (h + 1) * head)
        pieces = []
        if h > 0:
            pieces.append(jnp.zeros((h * head, cands), jnp.bfloat16))
        pieces.append(query[rows, :])
        if h < H - 1:
            pieces.append(jnp.zeros((embed - (h + 1) * head, cands), jnp.bfloat16))
        qpad[h] = jnp.concatenate(pieces, axis=0)
    acc[user] = jnp.zeros(acc.shape[1:], jnp.float32)
    top[...] = jnp.full(top.shape, LOW, jnp.float32)
    total[...] = jnp.zeros(total.shape, jnp.float32)

    @pl.loop(0, (count + PAIR - 1) // PAIR)
    def _(step):
        rows, biases = [], []
        places = lax.broadcasted_iota(jnp.int32, (BLOCK, 128), 0)
        for k in range(PAIR):
            at = step * PAIR + k
            inside = at < count
            block = jnp.where(inside, live[jnp.minimum(at, count - 1)], 0)
            limit = jnp.where(inside, length - (block + first) * BLOCK, 0)
            rows.append(hist[0, pl.ds(pl.multiple_of(block * BLOCK, BLOCK), BLOCK), :])
            biases.append(jnp.where(places < limit, 0.0, LOW))
        rows = jnp.concatenate(rows, axis=0)
        bias = jnp.concatenate(biases, axis=0)
        bias = jnp.concatenate([bias] * (cands // 128), axis=1)
        keys = jnp.dot(rows, weights[1], preferred_element_type=jnp.float32).astype(jnp.bfloat16)
        values = lax.dot_general(
            weights[2], rows, (((0,), (1,)), ((), ())), preferred_element_type=jnp.float32
        ).astype(jnp.bfloat16)
        for h in range(H):
            scores = jnp.dot(keys, qpad[h], preferred_element_type=jnp.float32) + bias
            before = top[h : h + 1, :]
            peak = jnp.maximum(before, jnp.max(scores, axis=0, keepdims=True))
            expo = jnp.exp2((scores - peak) * factor)
            shrink = jnp.exp2((before - peak) * factor)
            top[h : h + 1, :] = peak
            total[h : h + 1, :] = total[h : h + 1, :] * shrink + jnp.sum(expo, axis=0, keepdims=True)
            part = jnp.dot(
                values[h * head : (h + 1) * head, :],
                expo.astype(jnp.bfloat16),
                preferred_element_type=jnp.float32,
            )
            acc[user, h * head : (h + 1) * head, :] = acc[user, h * head : (h + 1) * head, :] * shrink + part

    for h in range(H):
        amount = total[h : h + 1, :]
        some = amount > 0.0
        safe = jnp.where(some, amount, 1.0)
        acc[user, h * head : (h + 1) * head, :] = acc[user, h * head : (h + 1) * head, :] * (1.0 / safe)
        lse[user, h : h + 1, :] = jnp.where(some, top[h : h + 1, :] * factor + jnp.log2(safe), LOW)

    @pl.when(user == users - 1)
    def _():
        for dest in range(parts.shape[0]):
            at = slice(dest * own_cands, (dest + 1) * own_cands)
            for u in range(acc.shape[0]):
                to = slice(u * own_cands, (u + 1) * own_cands)
                parts[dest, :, to] = acc[u, :, at].astype(jnp.bfloat16)
                stats[dest, :, to] = lse[u, :, at]


def combine_kernel(n, parts, stats, out_weight, result, got, got_stats, send_a, recv_a, send_b, recv_b):
    me = lax.axis_index("hist")
    barrier = pltpu.get_barrier_semaphore()
    for k in range(1, n):
        pl.semaphore_signal(
            barrier, inc=1, device_id={"hist": lax.rem(me + k, n)}, device_id_type=pl.DeviceIdType.MESH
        )
    pl.semaphore_wait(barrier, n - 1)
    copies = []
    for k in range(1, n):
        peer = lax.rem(me + k, n)
        for src, dst, send, recv in ((stats, got_stats, send_b, recv_b), (parts, got, send_a, recv_a)):
            copy = pltpu.make_async_remote_copy(
                src_ref=src.at[peer],
                dst_ref=dst.at[k - 1],
                send_sem=send.at[k - 1],
                recv_sem=recv.at[k - 1],
                device_id={"hist": peer},
                device_id_type=pl.DeviceIdType.MESH,
            )
            copy.start()
            copies.append(copy)
    for copy in copies:
        copy.wait()
    logs = [stats[me]] + [got_stats[k] for k in range(n - 1)]
    highest = functools.reduce(jnp.maximum, logs)
    shares = [jnp.exp2(log - highest) for log in logs]
    inverse = 1.0 / functools.reduce(jnp.add, shares)
    embed = parts.shape[1]
    head = embed // H
    pieces = []
    for h in range(H):
        rows = slice(h * head, (h + 1) * head)
        mixed = parts[me, rows, :].astype(jnp.float32) * shares[0][h : h + 1, :]
        for k in range(n - 1):
            mixed += got[k, rows, :].astype(jnp.float32) * shares[k + 1][h : h + 1, :]
        pieces.append(mixed * inverse[h : h + 1, :])
    attended = jnp.concatenate(pieces, axis=0).astype(jnp.bfloat16)
    result[...] = lax.dot_general(
        attended, out_weight[...], (((0,), (0,)), ((), ())), preferred_element_type=jnp.float32
    ).astype(jnp.bfloat16)


def body(candidates, history, projections, lengths, selected):
    n = lax.axis_size("hist")
    weights = lax.all_gather(projections, "dp", axis=1, tiled=True)
    whole = lax.all_gather(candidates, "hist", axis=1, tiled=True)
    users, own_cands, embed = candidates.shape
    cands = whole.shape[1]
    own_rows = history.shape[1]
    wide = -(-users * own_cands // 128) * 128
    base = (lax.axis_index("hist") * (own_rows // BLOCK)).astype(jnp.int32).reshape(1)
    parts, stats = pl.pallas_call(
        functools.partial(attend_kernel, own_cands),
        grid_spec=pltpu.PrefetchScalarGridSpec(
            num_scalar_prefetch=3,
            grid=(users,),
            in_specs=[
                pl.BlockSpec((1, cands, embed), lambda u, *_: (u, 0, 0)),
                pl.BlockSpec((1, own_rows, embed), lambda u, *_: (u, 0, 0)),
                pl.BlockSpec((4, embed, embed), lambda u, *_: (0, 0, 0)),
            ],
            out_specs=[
                pl.BlockSpec((n, embed, wide), lambda u, *_: (0, 0, 0)),
                pl.BlockSpec((n, H, wide), lambda u, *_: (0, 0, 0)),
            ],
            scratch_shapes=[
                pltpu.VMEM((H, embed, cands), jnp.bfloat16),
                pltpu.VMEM((users, embed, cands), jnp.float32),
                pltpu.VMEM((8, cands), jnp.float32),
                pltpu.VMEM((8, cands), jnp.float32),
                pltpu.VMEM((users, H, cands), jnp.float32),
                pltpu.SMEM((selected.shape[1] + 8,), jnp.int32),
            ],
        ),
        out_shape=[
            jax.ShapeDtypeStruct((n, embed, wide), jnp.bfloat16),
            jax.ShapeDtypeStruct((n, H, wide), jnp.float32),
        ],
        name="attend",
    )(lengths, selected, base, whole, history, weights)
    result = pl.pallas_call(
        functools.partial(combine_kernel, n),
        out_shape=jax.ShapeDtypeStruct((wide, embed), jnp.bfloat16),
        in_specs=[pl.BlockSpec(memory_space=pltpu.VMEM)] * 3,
        out_specs=pl.BlockSpec(memory_space=pltpu.VMEM),
        scratch_shapes=[
            pltpu.VMEM((n - 1, embed, wide), jnp.bfloat16),
            pltpu.VMEM((n - 1, H, wide), jnp.float32),
        ]
        + [pltpu.SemaphoreType.DMA((n - 1,))] * 4,
        compiler_params=pltpu.CompilerParams(collective_id=0, has_side_effects=True),
        name="combine",
    )(parts, stats, weights[3])
    return result[: users * own_cands].reshape(users, own_cands, embed)


def solution(mesh):
    placed = (
        P("dp", "hist", None),
        P("dp", "hist", None),
        P(None, "dp", None),
        P("dp"),
        P("dp", None),
    )
    return jax.shard_map(
        body, mesh=mesh, in_specs=placed, out_specs=P("dp", "hist", None), check_vma=False
    )
```

```python
import functools
import math

import jax
import jax.numpy as jnp
from jax import lax
from jax.experimental import pallas as pl
from jax.experimental.pallas import tpu as pltpu
from jax.sharding import PartitionSpec as P

H = 4
BLOCK = 128
PAIR = 2
LOW = -1e30


def gather_kernel(
    n, ranks, cand, proj, all_cand, all_proj, own_sem, z_send, z_recv, y_send, y_recv, w_send, w_recv
):
    mesh_id = pl.DeviceIdType.MESH
    me, rank = lax.axis_index("hist"), lax.axis_index("dp")
    line = n // 2
    side, spot = lax.rem(me, 2), me // 2
    users, own = cand.shape[0], cand.shape[1]
    rows = proj.shape[1]
    partner = spot * 2 + (1 - side)
    peers = [lax.rem(spot + k, line) * 2 + side for k in range(1, line)]
    mates = [lax.rem(rank + k, ranks) for k in range(1, ranks)]

    barrier = pltpu.get_barrier_semaphore()
    for peer in [partner] + peers:
        pl.semaphore_signal(barrier, inc=1, device_id={"hist": peer}, device_id_type=mesh_id)
    for mate in mates:
        pl.semaphore_signal(barrier, inc=1, device_id={"dp": mate}, device_id_type=mesh_id)
    pl.semaphore_wait(barrier, line + ranks - 1)

    def place(u, owner):
        return all_cand.at[u, pl.ds(pl.multiple_of(owner * own, own), own), :]

    strip = all_proj.at[:, pl.ds(pl.multiple_of(rank * rows, rows), rows), :]
    weight_copies = []
    for k, mate in enumerate(mates):
        copy = pltpu.make_async_remote_copy(
            proj, strip, w_send.at[k], w_recv.at[k], device_id={"dp": mate}, device_id_type=mesh_id
        )
        copy.start()
        weight_copies.append(copy)
    across, along = [], {}
    for u in range(users):
        for k, peer in enumerate(peers):
            copy = pltpu.make_async_remote_copy(
                cand.at[u],
                place(u, me),
                z_send.at[k, u],
                z_recv.at[k, u],
                device_id={"hist": peer},
                device_id_type=mesh_id,
            )
            copy.start()
            along[k, u] = copy
        copy = pltpu.make_async_remote_copy(
            cand.at[u],
            place(u, me),
            y_send.at[0, u],
            y_recv.at[0, u],
            device_id={"hist": partner},
            device_id_type=mesh_id,
        )
        copy.start()
        across.append(copy)
    locals_ = [pltpu.make_async_copy(proj, strip, own_sem.at[users])]
    locals_ += [pltpu.make_async_copy(cand.at[u], place(u, me), own_sem.at[u]) for u in range(users)]
    for copy in locals_:
        copy.start()
    for u in range(users):
        for k in range(line - 1):
            along[k, u].wait_recv()
            source = lax.rem(spot + line - (k + 1), line) * 2 + side
            copy = pltpu.make_async_remote_copy(
                place(u, source),
                place(u, source),
                y_send.at[k + 1, u],
                y_recv.at[k + 1, u],
                device_id={"hist": partner},
                device_id_type=mesh_id,
            )
            copy.start()
            across.append(copy)
    for copy in along.values():
        copy.wait_send()
    for copy in across + weight_copies + locals_:
        copy.wait()


def attend_kernel(
    own_cands,
    lengths,
    selected,
    base,
    cand,
    hist,
    weights,
    parts,
    stats,
    qpad,
    keys,
    values,
    acc,
    top,
    mean,
    lse,
    live,
):
    user = pl.program_id(0)
    users = pl.num_programs(0)
    cands, embed = cand.shape[1], cand.shape[2]
    head = embed // H
    tall = values.shape[1]
    factor = math.log2(math.e) / math.sqrt(head)
    blocks = hist.shape[1] // BLOCK
    length = lengths[user]
    first = base[0]
    chosen = selected.shape[1]

    def note(j, count):
        block = selected[user, j] - first
        live[count] = block
        ok = jnp.logical_and(block >= 0, block < blocks)
        ok = jnp.logical_and(ok, (block + first) * BLOCK < length)
        return count + jnp.where(ok, 1, 0)

    def note_many(j, count):
        for step in range(8):
            count = note(j * 8 + step, count)
        return count

    count = lax.fori_loop(0, chosen // 8, note_many, jnp.int32(0))

    query = lax.dot_general(
        weights[0], cand[0], (((0,), (1,)), ((), ())), preferred_element_type=jnp.float32
    ).astype(jnp.bfloat16)
    for h in range(H):
        rows = slice(h * head, (h + 1) * head)
        pieces = []
        if h > 0:
            pieces.append(jnp.zeros((h * head, cands), jnp.bfloat16))
        pieces.append(query[rows, :])
        if h < H - 1:
            pieces.append(jnp.zeros((embed - (h + 1) * head, cands), jnp.bfloat16))
        qpad[h] = jnp.concatenate(pieces, axis=0)
    down = lax.broadcasted_iota(jnp.int32, (BLOCK, embed), 0)
    right = lax.broadcasted_iota(jnp.int32, (tall - head, BLOCK), 1)
    under = lax.broadcasted_iota(jnp.int32, (tall - head, BLOCK), 0)
    for b in range(blocks):
        limit = length - (first + b) * BLOCK
        span = slice(b * BLOCK, (b + 1) * BLOCK)
        rows = hist[0, span, :]
        alive = down < limit
        safe = jnp.where(alive, rows.astype(jnp.float32), rows[0:1, :].astype(jnp.float32)).astype(jnp.bfloat16)
        kept = jnp.where(alive, rows.astype(jnp.float32), 0.0).astype(jnp.bfloat16)
        keys[span, :] = jnp.dot(safe, weights[1], preferred_element_type=jnp.float32).astype(jnp.bfloat16)
        turned = lax.dot_general(
            weights[2], kept, (((0,), (1,)), ((), ())), preferred_element_type=jnp.float32
        ).astype(jnp.bfloat16)
        ones = jnp.where(jnp.logical_and(right < limit, under == 0), 1.0, 0.0).astype(jnp.bfloat16)
        for h in range(H):
            values[h, 0:head, span] = turned[h * head : (h + 1) * head, :]
            values[h, head:tall, span] = ones
    acc[...] = jnp.zeros(acc.shape, jnp.float32)
    top[...] = jnp.full(top.shape, LOW, jnp.float32)

    @pl.loop(0, (count + PAIR - 1) // PAIR)
    def _(step):
        starts, flags = [], []
        for k in range(PAIR):
            at = step * PAIR + k
            block = live[jnp.minimum(at, count - 1)]
            starts.append(pl.ds(pl.multiple_of(block * BLOCK, BLOCK), BLOCK))
            flags.append(jnp.where(at < count, 1.0, 0.0).astype(jnp.bfloat16))
        key = jnp.concatenate([keys[at, :] for at in starts], axis=0)
        for h in range(H):
            scores = jnp.dot(key, qpad[h], preferred_element_type=jnp.float32)
            before = top[h : h + 1, :]
            peak = jnp.maximum(before, jnp.max(scores, axis=0, keepdims=True))
            expo = jnp.exp2((scores - peak) * factor).astype(jnp.bfloat16)
            shrink = jnp.exp2((before - peak) * factor)
            top[h : h + 1, :] = peak
            value = jnp.concatenate([values[h, :, at] * flag for at, flag in zip(starts, flags)], axis=1)
            acc[h] = acc[h] * shrink + jnp.dot(value, expo, preferred_element_type=jnp.float32)

    for h in range(H):
        amount = acc[h, head : head + 1, :]
        some = amount > 0.0
        safe = jnp.where(some, amount, 1.0)
        mean[user, h * head : (h + 1) * head, :] = (acc[h, 0:head, :] * (1.0 / safe)).astype(jnp.bfloat16)
        lse[user, h : h + 1, :] = jnp.where(some, top[h : h + 1, :] * factor + jnp.log2(safe), LOW)

    @pl.when(user == users - 1)
    def _():
        for dest in range(parts.shape[0]):
            at = slice(dest * own_cands, (dest + 1) * own_cands)
            for u in range(mean.shape[0]):
                to = slice(u * own_cands, (u + 1) * own_cands)
                parts[dest, :, to] = mean[u, :, at]
                stats[dest, :, to] = lse[u, :, at]


def combine_kernel(n, parts, stats, out_weight, result, got, got_stats, send_a, recv_a, send_b, recv_b):
    me = lax.axis_index("hist")
    barrier = pltpu.get_barrier_semaphore()
    for k in range(1, n):
        pl.semaphore_signal(
            barrier, inc=1, device_id={"hist": lax.rem(me + k, n)}, device_id_type=pl.DeviceIdType.MESH
        )
    pl.semaphore_wait(barrier, n - 1)
    copies = []
    for k in range(1, n):
        peer = lax.rem(me + k, n)
        for src, dst, send, recv in ((stats, got_stats, send_b, recv_b), (parts, got, send_a, recv_a)):
            copy = pltpu.make_async_remote_copy(
                src_ref=src.at[peer],
                dst_ref=dst.at[k - 1],
                send_sem=send.at[k - 1],
                recv_sem=recv.at[k - 1],
                device_id={"hist": peer},
                device_id_type=pl.DeviceIdType.MESH,
            )
            copy.start()
            copies.append(copy)
    for copy in copies:
        copy.wait()
    logs = [stats[me]] + [got_stats[k] for k in range(n - 1)]
    highest = functools.reduce(jnp.maximum, logs)
    shares = [jnp.exp2(log - highest) for log in logs]
    inverse = 1.0 / functools.reduce(jnp.add, shares)
    embed = parts.shape[1]
    head = embed // H
    pieces = []
    for h in range(H):
        rows = slice(h * head, (h + 1) * head)
        mixed = parts[me, rows, :].astype(jnp.float32) * shares[0][h : h + 1, :]
        for k in range(n - 1):
            mixed += got[k, rows, :].astype(jnp.float32) * shares[k + 1][h : h + 1, :]
        pieces.append(mixed * inverse[h : h + 1, :])
    attended = jnp.concatenate(pieces, axis=0).astype(jnp.bfloat16)
    result[...] = lax.dot_general(
        attended, out_weight[3], (((0,), (0,)), ((), ())), preferred_element_type=jnp.float32
    ).astype(jnp.bfloat16)


def body(candidates, history, projections, lengths, selected):
    n = lax.axis_size("hist")
    ranks = lax.axis_size("dp")
    users, own_cands, embed = candidates.shape
    cands = n * own_cands
    line = n // 2
    whole, weights = pl.pallas_call(
        functools.partial(gather_kernel, n, ranks),
        out_shape=[
            jax.ShapeDtypeStruct((users, cands, embed), jnp.bfloat16),
            jax.ShapeDtypeStruct((projections.shape[0], ranks * projections.shape[1], embed), jnp.bfloat16),
        ],
        in_specs=[pl.BlockSpec(memory_space=pltpu.VMEM)] * 2,
        out_specs=[pl.BlockSpec(memory_space=pltpu.VMEM)] * 2,
        scratch_shapes=[
            pltpu.SemaphoreType.DMA((users + 1,)),
            pltpu.SemaphoreType.DMA((line - 1, users)),
            pltpu.SemaphoreType.DMA((line - 1, users)),
            pltpu.SemaphoreType.DMA((line, users)),
            pltpu.SemaphoreType.DMA((line, users)),
            pltpu.SemaphoreType.DMA((ranks - 1,)),
            pltpu.SemaphoreType.DMA((ranks - 1,)),
        ],
        compiler_params=pltpu.CompilerParams(collective_id=1, has_side_effects=True),
        name="gather",
    )(candidates, projections)
    own_rows = history.shape[1]
    wide = -(-users * own_cands // 128) * 128
    base = (lax.axis_index("hist") * (own_rows // BLOCK)).astype(jnp.int32).reshape(1)
    parts, stats = pl.pallas_call(
        functools.partial(attend_kernel, own_cands),
        grid_spec=pltpu.PrefetchScalarGridSpec(
            num_scalar_prefetch=3,
            grid=(users,),
            in_specs=[
                pl.BlockSpec((1, cands, embed), lambda u, *_: (u, 0, 0)),
                pl.BlockSpec((1, own_rows, embed), lambda u, *_: (u, 0, 0)),
                pl.BlockSpec((4, embed, embed), lambda u, *_: (0, 0, 0)),
            ],
            out_specs=[
                pl.BlockSpec((n, embed, wide), lambda u, *_: (0, 0, 0)),
                pl.BlockSpec((n, H, wide), lambda u, *_: (0, 0, 0)),
            ],
            scratch_shapes=[
                pltpu.VMEM((H, embed, cands), jnp.bfloat16),
                pltpu.VMEM((own_rows, embed), jnp.bfloat16),
                pltpu.VMEM((H, embed // H + 16, own_rows), jnp.bfloat16),
                pltpu.VMEM((H, embed // H + 16, cands), jnp.float32),
                pltpu.VMEM((8, cands), jnp.float32),
                pltpu.VMEM((users, embed, cands), jnp.bfloat16),
                pltpu.VMEM((users, H, cands), jnp.float32),
                pltpu.SMEM((selected.shape[1] + 8,), jnp.int32),
            ],
        ),
        out_shape=[
            jax.ShapeDtypeStruct((n, embed, wide), jnp.bfloat16),
            jax.ShapeDtypeStruct((n, H, wide), jnp.float32),
        ],
        name="attend",
    )(lengths, selected, base, whole, history, weights)
    result = pl.pallas_call(
        functools.partial(combine_kernel, n),
        out_shape=jax.ShapeDtypeStruct((wide, embed), jnp.bfloat16),
        in_specs=[pl.BlockSpec(memory_space=pltpu.VMEM)] * 3,
        out_specs=pl.BlockSpec(memory_space=pltpu.VMEM),
        scratch_shapes=[
            pltpu.VMEM((n - 1, embed, wide), jnp.bfloat16),
            pltpu.VMEM((n - 1, H, wide), jnp.float32),
        ]
        + [pltpu.SemaphoreType.DMA((n - 1,))] * 4,
        compiler_params=pltpu.CompilerParams(collective_id=0, has_side_effects=True),
        name="combine",
    )(parts, stats, weights)
    return result[: users * own_cands].reshape(users, own_cands, embed)


def solution(mesh):
    placed = (
        P("dp", "hist", None),
        P("dp", "hist", None),
        P(None, "dp", None),
        P("dp"),
        P("dp", None),
    )
    return jax.shard_map(
        body, mesh=mesh, in_specs=placed, out_specs=P("dp", "hist", None), check_vma=False
    )
```

```python
import functools
import math

import jax
import jax.numpy as jnp
from jax import lax
from jax.experimental import pallas as pl
from jax.experimental.pallas import tpu as pltpu
from jax.sharding import PartitionSpec as P

H = 4
BLOCK = 128
PAIR = 2
LOW = -1e30


def gather_kernel(
    n,
    ranks,
    lengths,
    cand,
    proj,
    hist,
    all_cand,
    all_proj,
    all_keys,
    all_values,
    rows_in,
    keys,
    values,
    own_sem,
    in_sem,
    out_sem,
    z_send,
    z_recv,
    y_send,
    y_recv,
    w_send,
    w_recv,
):
    mesh_id = pl.DeviceIdType.MESH
    me, rank = lax.axis_index("hist"), lax.axis_index("dp")
    line = n // 2
    side, spot = lax.rem(me, 2), me // 2
    users, own = cand.shape[0], cand.shape[1]
    rows = proj.shape[1]
    own_rows, embed = hist.shape[1], hist.shape[2]
    blocks = own_rows // BLOCK
    fetches = [pltpu.make_async_copy(hist.at[u], rows_in.at[u], in_sem.at[u]) for u in range(users)]
    for copy in fetches:
        copy.start()
    partner = spot * 2 + (1 - side)
    peers = [lax.rem(spot + k, line) * 2 + side for k in range(1, line)]
    mates = [lax.rem(rank + k, ranks) for k in range(1, ranks)]

    barrier = pltpu.get_barrier_semaphore()
    for peer in [partner] + peers:
        pl.semaphore_signal(barrier, inc=1, device_id={"hist": peer}, device_id_type=mesh_id)
    for mate in mates:
        pl.semaphore_signal(barrier, inc=1, device_id={"dp": mate}, device_id_type=mesh_id)
    pl.semaphore_wait(barrier, line + ranks - 1)

    def place(u, owner):
        return all_cand.at[u, pl.ds(pl.multiple_of(owner * own, own), own), :]

    strip = all_proj.at[:, pl.ds(pl.multiple_of(rank * rows, rows), rows), :]
    weight_copies = []
    for k, mate in enumerate(mates):
        copy = pltpu.make_async_remote_copy(
            proj, strip, w_send.at[k], w_recv.at[k], device_id={"dp": mate}, device_id_type=mesh_id
        )
        copy.start()
        weight_copies.append(copy)
    across, along = [], {}
    for u in range(users):
        for k, peer in enumerate(peers):
            copy = pltpu.make_async_remote_copy(
                cand.at[u],
                place(u, me),
                z_send.at[k, u],
                z_recv.at[k, u],
                device_id={"hist": peer},
                device_id_type=mesh_id,
            )
            copy.start()
            along[k, u] = copy
        copy = pltpu.make_async_remote_copy(
            cand.at[u],
            place(u, me),
            y_send.at[0, u],
            y_recv.at[0, u],
            device_id={"hist": partner},
            device_id_type=mesh_id,
        )
        copy.start()
        across.append(copy)
    locals_ = [pltpu.make_async_copy(proj, strip, own_sem.at[users])]
    locals_ += [pltpu.make_async_copy(cand.at[u], place(u, me), own_sem.at[u]) for u in range(users)]
    for copy in locals_:
        copy.start()
    locals_[0].wait()
    for copy in weight_copies:
        copy.wait()
    key_weight, value_weight = all_proj[1], all_proj[2]
    shape = (blocks, BLOCK, embed)
    places = lax.broadcasted_iota(jnp.int32, shape, 0) * BLOCK + lax.broadcasted_iota(jnp.int32, shape, 1)
    places = places + me * own_rows
    stores = []
    for u in range(users):
        for k in range(line - 1):
            along[k, u].wait_recv()
            source = lax.rem(spot + line - (k + 1), line) * 2 + side
            copy = pltpu.make_async_remote_copy(
                place(u, source),
                place(u, source),
                y_send.at[k + 1, u],
                y_recv.at[k + 1, u],
                device_id={"hist": partner},
                device_id_type=mesh_id,
            )
            copy.start()
            across.append(copy)
        fetches[u].wait()
        block_rows = rows_in[u].reshape(shape).astype(jnp.float32)
        alive = places < lengths[u]
        safe = jnp.where(alive, block_rows, block_rows[:, 0:1, :]).astype(jnp.bfloat16).reshape(own_rows, embed)
        kept = jnp.where(alive, block_rows, 0.0).astype(jnp.bfloat16).reshape(own_rows, embed)
        keys[u] = jnp.dot(safe, key_weight, preferred_element_type=jnp.float32).astype(jnp.bfloat16)
        values[u] = lax.dot_general(
            value_weight, kept, (((0,), (1,)), ((), ())), preferred_element_type=jnp.float32
        ).astype(jnp.bfloat16)
        for k, (src, dst) in enumerate(((keys, all_keys), (values, all_values))):
            copy = pltpu.make_async_copy(src.at[u], dst.at[u], out_sem.at[k, u])
            copy.start()
            stores.append(copy)
    for copy in along.values():
        copy.wait_send()
    for copy in across + locals_[1:] + stores:
        copy.wait()


def attend_kernel(
    own_cands,
    lengths,
    flags,
    base,
    cand,
    keys,
    values,
    weights,
    parts,
    stats,
    qpad,
    acc,
    top,
    mean,
    lse,
    live,
):
    user = pl.program_id(0)
    users = pl.num_programs(0)
    cands, embed = cand.shape[1], cand.shape[2]
    head = embed // H
    tall = acc.shape[1]
    factor = math.log2(math.e) / math.sqrt(head)
    length = lengths[user]
    first = base[0]
    count = jnp.int32(0)
    for b in range(keys.shape[1] // BLOCK):
        live[count] = b
        count = count + flags[user, b]

    query = lax.dot_general(
        weights[0], cand[0], (((0,), (1,)), ((), ())), preferred_element_type=jnp.float32
    ).astype(jnp.bfloat16)
    for h in range(H):
        rows = slice(h * head, (h + 1) * head)
        pieces = []
        if h > 0:
            pieces.append(jnp.zeros((h * head, cands), jnp.bfloat16))
        pieces.append(query[rows, :])
        if h < H - 1:
            pieces.append(jnp.zeros((embed - (h + 1) * head, cands), jnp.bfloat16))
        qpad[h] = jnp.concatenate(pieces, axis=0)
    acc[...] = jnp.zeros(acc.shape, jnp.float32)
    top[...] = jnp.full(top.shape, LOW, jnp.float32)

    right = lax.broadcasted_iota(jnp.int32, (tall - head, BLOCK), 1)
    under = lax.broadcasted_iota(jnp.int32, (tall - head, BLOCK), 0)
    right = jnp.where(under == 0, right, jnp.iinfo(jnp.int32).max)

    def visit(begin, many):
        starts, ones = [], []
        for k in range(many):
            block = live[begin + k]
            starts.append(pl.ds(pl.multiple_of(block * BLOCK, BLOCK), BLOCK))
            ones.append(jnp.where(right < length - (block + first) * BLOCK, 1.0, 0.0).astype(jnp.bfloat16))
        key = jnp.concatenate([keys[0, at, :] for at in starts], axis=0)
        one = jnp.concatenate(ones, axis=1)
        for h in range(H):
            scores = jnp.dot(key, qpad[h], preferred_element_type=jnp.float32)
            before = top[h : h + 1, :]
            peak = jnp.maximum(before, jnp.max(scores, axis=0, keepdims=True))
            expo = jnp.exp2((scores - peak) * factor).astype(jnp.bfloat16)
            shrink = jnp.exp2((before - peak) * factor)
            top[h : h + 1, :] = peak
            value = jnp.concatenate([values[0, h * head : (h + 1) * head, at] for at in starts], axis=1)
            value = jnp.concatenate([value, one], axis=0)
            acc[h] = acc[h] * shrink + jnp.dot(value, expo, preferred_element_type=jnp.float32)

    @pl.loop(0, count // PAIR)
    def _(step):
        visit(step * PAIR, PAIR)

    @pl.when(count % PAIR == 1)
    def _():
        visit(count - 1, 1)

    for h in range(H):
        amount = acc[h, head : head + 1, :]
        some = amount > 0.0
        safe = jnp.where(some, amount, 1.0)
        mean[user, h * head : (h + 1) * head, :] = (acc[h, 0:head, :] * (1.0 / safe)).astype(jnp.bfloat16)
        lse[user, h : h + 1, :] = jnp.where(some, top[h : h + 1, :] * factor + jnp.log2(safe), LOW)

    @pl.when(user == users - 1)
    def _():
        for dest in range(parts.shape[0]):
            at = slice(dest * own_cands, (dest + 1) * own_cands)
            for u in range(mean.shape[0]):
                to = slice(u * own_cands, (u + 1) * own_cands)
                parts[dest, :, to] = mean[u, :, at]
                stats[dest, :, to] = lse[u, :, at]


def combine_kernel(n, parts, stats, out_weight, result, got, got_stats, send_a, recv_a, send_b, recv_b):
    me = lax.axis_index("hist")
    barrier = pltpu.get_barrier_semaphore()
    for k in range(1, n):
        pl.semaphore_signal(
            barrier, inc=1, device_id={"hist": lax.rem(me + k, n)}, device_id_type=pl.DeviceIdType.MESH
        )
    pl.semaphore_wait(barrier, n - 1)
    copies = []
    for k in range(1, n):
        peer = lax.rem(me + k, n)
        for src, dst, send, recv in ((stats, got_stats, send_b, recv_b), (parts, got, send_a, recv_a)):
            copy = pltpu.make_async_remote_copy(
                src_ref=src.at[peer],
                dst_ref=dst.at[k - 1],
                send_sem=send.at[k - 1],
                recv_sem=recv.at[k - 1],
                device_id={"hist": peer},
                device_id_type=pl.DeviceIdType.MESH,
            )
            copy.start()
            copies.append(copy)
    for copy in copies:
        copy.wait()
    logs = [stats[me]] + [got_stats[k] for k in range(n - 1)]
    highest = functools.reduce(jnp.maximum, logs)
    shares = [jnp.exp2(log - highest) for log in logs]
    inverse = 1.0 / functools.reduce(jnp.add, shares)
    embed = parts.shape[1]
    head = embed // H
    pieces = []
    for h in range(H):
        rows = slice(h * head, (h + 1) * head)
        mixed = parts[me, rows, :].astype(jnp.float32) * shares[0][h : h + 1, :]
        for k in range(n - 1):
            mixed += got[k, rows, :].astype(jnp.float32) * shares[k + 1][h : h + 1, :]
        pieces.append(mixed * inverse[h : h + 1, :])
    attended = jnp.concatenate(pieces, axis=0).astype(jnp.bfloat16)
    result[...] = lax.dot_general(
        attended, out_weight[3], (((0,), (0,)), ((), ())), preferred_element_type=jnp.float32
    ).astype(jnp.bfloat16)


def body(candidates, history, projections, lengths, selected):
    n = lax.axis_size("hist")
    ranks = lax.axis_size("dp")
    users, own_cands, embed = candidates.shape
    cands = n * own_cands
    line = n // 2
    own_rows = history.shape[1]
    blocks = own_rows // BLOCK
    first = (lax.axis_index("hist") * blocks).astype(jnp.int32)
    ids = first + jnp.arange(blocks, dtype=jnp.int32)
    flags = jnp.any(selected[:, :, None] == ids[None, None, :], axis=1)
    flags = jnp.logical_and(flags, ids[None, :] * BLOCK < lengths[:, None]).astype(jnp.int32)
    base = first.reshape(1)
    whole, weights, keys, values = pl.pallas_call(
        functools.partial(gather_kernel, n, ranks),
        out_shape=[
            jax.ShapeDtypeStruct((users, cands, embed), jnp.bfloat16),
            jax.ShapeDtypeStruct((projections.shape[0], ranks * projections.shape[1], embed), jnp.bfloat16),
            jax.ShapeDtypeStruct((users, own_rows, embed), jnp.bfloat16),
            jax.ShapeDtypeStruct((users, embed, own_rows), jnp.bfloat16),
        ],
        in_specs=[pl.BlockSpec(memory_space=pltpu.SMEM)]
        + [pl.BlockSpec(memory_space=pltpu.VMEM)] * 2
        + [pl.BlockSpec(memory_space=pl.ANY)],
        out_specs=[pl.BlockSpec(memory_space=pltpu.VMEM)] * 2 + [pl.BlockSpec(memory_space=pl.ANY)] * 2,
        scratch_shapes=[
            pltpu.VMEM((users, own_rows, embed), jnp.bfloat16),
            pltpu.VMEM((users, own_rows, embed), jnp.bfloat16),
            pltpu.VMEM((users, embed, own_rows), jnp.bfloat16),
            pltpu.SemaphoreType.DMA((users + 1,)),
            pltpu.SemaphoreType.DMA((users,)),
            pltpu.SemaphoreType.DMA((2, users)),
            pltpu.SemaphoreType.DMA((line - 1, users)),
            pltpu.SemaphoreType.DMA((line - 1, users)),
            pltpu.SemaphoreType.DMA((line, users)),
            pltpu.SemaphoreType.DMA((line, users)),
            pltpu.SemaphoreType.DMA((ranks - 1,)),
            pltpu.SemaphoreType.DMA((ranks - 1,)),
        ],
        compiler_params=pltpu.CompilerParams(collective_id=1, has_side_effects=True),
        name="gather",
    )(lengths, candidates, projections, history)
    wide = -(-users * own_cands // 128) * 128
    parts, stats = pl.pallas_call(
        functools.partial(attend_kernel, own_cands),
        grid_spec=pltpu.PrefetchScalarGridSpec(
            num_scalar_prefetch=3,
            grid=(users,),
            in_specs=[
                pl.BlockSpec((1, cands, embed), lambda u, *_: (u, 0, 0)),
                pl.BlockSpec((1, own_rows, embed), lambda u, *_: (u, 0, 0)),
                pl.BlockSpec((1, embed, own_rows), lambda u, *_: (u, 0, 0)),
                pl.BlockSpec((4, embed, embed), lambda u, *_: (0, 0, 0)),
            ],
            out_specs=[
                pl.BlockSpec((n, embed, wide), lambda u, *_: (0, 0, 0)),
                pl.BlockSpec((n, H, wide), lambda u, *_: (0, 0, 0)),
            ],
            scratch_shapes=[
                pltpu.VMEM((H, embed, cands), jnp.bfloat16),
                pltpu.VMEM((H, embed // H + 16, cands), jnp.float32),
                pltpu.VMEM((8, cands), jnp.float32),
                pltpu.VMEM((users, embed, cands), jnp.bfloat16),
                pltpu.VMEM((users, H, cands), jnp.float32),
                pltpu.SMEM((blocks + 8,), jnp.int32),
            ],
        ),
        out_shape=[
            jax.ShapeDtypeStruct((n, embed, wide), jnp.bfloat16),
            jax.ShapeDtypeStruct((n, H, wide), jnp.float32),
        ],
        name="attend",
    )(lengths, flags, base, whole, keys, values, weights)
    result = pl.pallas_call(
        functools.partial(combine_kernel, n),
        out_shape=jax.ShapeDtypeStruct((wide, embed), jnp.bfloat16),
        in_specs=[pl.BlockSpec(memory_space=pltpu.VMEM)] * 3,
        out_specs=pl.BlockSpec(memory_space=pltpu.VMEM),
        scratch_shapes=[
            pltpu.VMEM((n - 1, embed, wide), jnp.bfloat16),
            pltpu.VMEM((n - 1, H, wide), jnp.float32),
        ]
        + [pltpu.SemaphoreType.DMA((n - 1,))] * 4,
        compiler_params=pltpu.CompilerParams(collective_id=0, has_side_effects=True),
        name="combine",
    )(parts, stats, weights)
    return result[: users * own_cands].reshape(users, own_cands, embed)


def solution(mesh):
    placed = (
        P("dp", "hist", None),
        P("dp", "hist", None),
        P(None, "dp", None),
        P("dp"),
        P("dp", None),
    )
    return jax.shard_map(
        body, mesh=mesh, in_specs=placed, out_specs=P("dp", "hist", None), check_vma=False
    )
```

```python
import functools
import math

import jax
import jax.numpy as jnp
from jax import lax
from jax.experimental import pallas as pl
from jax.experimental.pallas import tpu as pltpu
from jax.sharding import PartitionSpec as P

H = 4
BLOCK = 128
PAIR = 2
LOW = -1e30


def gather_kernel(
    n,
    ranks,
    lengths,
    cand,
    proj,
    hist,
    picks,
    all_cand,
    all_proj,
    all_keys,
    all_values,
    flags,
    rows_in,
    keys,
    values,
    own_sem,
    in_sem,
    out_sem,
    z_send,
    z_recv,
    y_send,
    y_recv,
    w_send,
    w_recv,
):
    mesh_id = pl.DeviceIdType.MESH
    me, rank = lax.axis_index("hist"), lax.axis_index("dp")
    line = n // 2
    side, spot = lax.rem(me, 2), me // 2
    users, own = cand.shape[0], cand.shape[1]
    rows = proj.shape[1]
    own_rows, embed = hist.shape[1], hist.shape[2]
    blocks = own_rows // BLOCK
    fetches = [pltpu.make_async_copy(hist.at[u], rows_in.at[u], in_sem.at[u]) for u in range(users)]
    for copy in fetches:
        copy.start()
    partner = spot * 2 + (1 - side)
    peers = [lax.rem(spot + k, line) * 2 + side for k in range(1, line)]
    mates = [lax.rem(rank + k, ranks) for k in range(1, ranks)]

    barrier = pltpu.get_barrier_semaphore()
    for peer in [partner] + peers:
        pl.semaphore_signal(barrier, inc=1, device_id={"hist": peer}, device_id_type=mesh_id)
    for mate in mates:
        pl.semaphore_signal(barrier, inc=1, device_id={"dp": mate}, device_id_type=mesh_id)
    pl.semaphore_wait(barrier, line + ranks - 1)

    def place(u, owner):
        return all_cand.at[u, pl.ds(pl.multiple_of(owner * own, own), own), :]

    strip = all_proj.at[:, pl.ds(pl.multiple_of(rank * rows, rows), rows), :]
    weight_copies = []
    for k, mate in enumerate(mates):
        copy = pltpu.make_async_remote_copy(
            proj, strip, w_send.at[k], w_recv.at[k], device_id={"dp": mate}, device_id_type=mesh_id
        )
        copy.start()
        weight_copies.append(copy)
    across, along = [], {}
    for u in range(users):
        for k, peer in enumerate(peers):
            copy = pltpu.make_async_remote_copy(
                cand.at[u],
                place(u, me),
                z_send.at[k, u],
                z_recv.at[k, u],
                device_id={"hist": peer},
                device_id_type=mesh_id,
            )
            copy.start()
            along[k, u] = copy
        copy = pltpu.make_async_remote_copy(
            cand.at[u],
            place(u, me),
            y_send.at[0, u],
            y_recv.at[0, u],
            device_id={"hist": partner},
            device_id_type=mesh_id,
        )
        copy.start()
        across.append(copy)
    locals_ = [pltpu.make_async_copy(proj, strip, own_sem.at[users])]
    locals_ += [pltpu.make_async_copy(cand.at[u], place(u, me), own_sem.at[u]) for u in range(users)]
    for copy in locals_:
        copy.start()
    spans = lax.broadcasted_iota(jnp.int32, (users, 128), 0)
    limits = jnp.zeros((users, 128), jnp.int32)
    for u in range(users):
        limits = jnp.where(spans == u, lengths[u], limits)
    lane = lax.broadcasted_iota(jnp.int32, (users, 128), 1)
    found = jnp.zeros((users, 128), jnp.int32)
    chosen = picks[...]
    for b in range(blocks):
        hit = jnp.max(jnp.where(chosen == me * blocks + b, 1.0, 0.0), axis=1, keepdims=True)
        found = jnp.where(jnp.logical_and(lane == b, hit > 0.0), 1, found)
    flags[...] = jnp.where((me * blocks + lane) * BLOCK < limits, found, 0)
    locals_[0].wait()
    for copy in weight_copies:
        copy.wait()
    key_weight, value_weight = all_proj[1], all_proj[2]
    shape = (blocks, BLOCK, embed)
    places = lax.broadcasted_iota(jnp.int32, shape, 0) * BLOCK + lax.broadcasted_iota(jnp.int32, shape, 1)
    places = places + me * own_rows
    stores = []
    for u in range(users):
        for k in range(line - 1):
            along[k, u].wait_recv()
            source = lax.rem(spot + line - (k + 1), line) * 2 + side
            copy = pltpu.make_async_remote_copy(
                place(u, source),
                place(u, source),
                y_send.at[k + 1, u],
                y_recv.at[k + 1, u],
                device_id={"hist": partner},
                device_id_type=mesh_id,
            )
            copy.start()
            across.append(copy)
        fetches[u].wait()
        block_rows = rows_in[u].reshape(shape).astype(jnp.float32)
        alive = places < lengths[u]
        safe = jnp.where(alive, block_rows, block_rows[:, 0:1, :]).astype(jnp.bfloat16).reshape(own_rows, embed)
        kept = jnp.where(alive, block_rows, 0.0).astype(jnp.bfloat16).reshape(own_rows, embed)
        keys[u] = jnp.dot(safe, key_weight, preferred_element_type=jnp.float32).astype(jnp.bfloat16)
        values[u] = lax.dot_general(
            value_weight, kept, (((0,), (1,)), ((), ())), preferred_element_type=jnp.float32
        ).astype(jnp.bfloat16)
        for k, (src, dst) in enumerate(((keys, all_keys), (values, all_values))):
            copy = pltpu.make_async_copy(src.at[u], dst.at[u], out_sem.at[k, u])
            copy.start()
            stores.append(copy)
    for copy in along.values():
        copy.wait_send()
    for copy in across + locals_[1:] + stores:
        copy.wait()


def attend_kernel(
    own_cands,
    lengths,
    flags,
    base,
    cand,
    keys,
    values,
    weights,
    parts,
    stats,
    qpad,
    acc,
    top,
    mean,
    lse,
    live,
):
    user = pl.program_id(0)
    users = pl.num_programs(0)
    cands, embed = cand.shape[1], cand.shape[2]
    head = embed // H
    tall = acc.shape[1]
    factor = math.log2(math.e) / math.sqrt(head)
    length = lengths[user]
    first = base[0]
    count = jnp.int32(0)
    for b in range(keys.shape[1] // BLOCK):
        live[count] = b
        count = count + flags[user, b]

    query = lax.dot_general(
        weights[0], cand[0], (((0,), (1,)), ((), ())), preferred_element_type=jnp.float32
    ).astype(jnp.bfloat16)
    for h in range(H):
        rows = slice(h * head, (h + 1) * head)
        pieces = []
        if h > 0:
            pieces.append(jnp.zeros((h * head, cands), jnp.bfloat16))
        pieces.append(query[rows, :])
        if h < H - 1:
            pieces.append(jnp.zeros((embed - (h + 1) * head, cands), jnp.bfloat16))
        qpad[h] = jnp.concatenate(pieces, axis=0)
    acc[...] = jnp.zeros(acc.shape, jnp.float32)
    top[...] = jnp.full(top.shape, LOW, jnp.float32)

    right = lax.broadcasted_iota(jnp.int32, (tall - head, BLOCK), 1)
    under = lax.broadcasted_iota(jnp.int32, (tall - head, BLOCK), 0)
    right = jnp.where(under == 0, right, jnp.iinfo(jnp.int32).max)

    def visit(begin, many):
        starts, ones = [], []
        for k in range(many):
            block = live[begin + k]
            starts.append(pl.ds(pl.multiple_of(block * BLOCK, BLOCK), BLOCK))
            ones.append(jnp.where(right < length - (block + first) * BLOCK, 1.0, 0.0).astype(jnp.bfloat16))
        key = jnp.concatenate([keys[0, at, :] for at in starts], axis=0)
        one = jnp.concatenate(ones, axis=1)
        for h in range(H):
            scores = jnp.dot(key, qpad[h], preferred_element_type=jnp.float32)
            before = top[h : h + 1, :]
            peak = jnp.maximum(before, jnp.max(scores, axis=0, keepdims=True))
            expo = jnp.exp2((scores - peak) * factor).astype(jnp.bfloat16)
            shrink = jnp.exp2((before - peak) * factor)
            top[h : h + 1, :] = peak
            value = jnp.concatenate([values[0, h * head : (h + 1) * head, at] for at in starts], axis=1)
            value = jnp.concatenate([value, one], axis=0)
            acc[h] = acc[h] * shrink + jnp.dot(value, expo, preferred_element_type=jnp.float32)

    @pl.loop(0, count // PAIR)
    def _(step):
        visit(step * PAIR, PAIR)

    @pl.when(count % PAIR == 1)
    def _():
        visit(count - 1, 1)

    for h in range(H):
        amount = acc[h, head : head + 1, :]
        some = amount > 0.0
        safe = jnp.where(some, amount, 1.0)
        mean[user, h * head : (h + 1) * head, :] = (acc[h, 0:head, :] * (1.0 / safe)).astype(jnp.bfloat16)
        lse[user, h : h + 1, :] = jnp.where(some, top[h : h + 1, :] * factor + jnp.log2(safe), LOW)

    @pl.when(user == users - 1)
    def _():
        for dest in range(parts.shape[0]):
            at = slice(dest * own_cands, (dest + 1) * own_cands)
            count_all = mean.shape[0]
            to = slice(0, count_all * own_cands)
            parts[dest, :, to] = jnp.concatenate([mean[u, :, at] for u in range(count_all)], axis=1)
            stats[dest, :, to] = jnp.concatenate([lse[u, :, at] for u in range(count_all)], axis=1)


def combine_kernel(n, parts, stats, out_weight, result, got, got_stats, send_a, recv_a, send_b, recv_b):
    me = lax.axis_index("hist")
    barrier = pltpu.get_barrier_semaphore()
    for k in range(1, n):
        pl.semaphore_signal(
            barrier, inc=1, device_id={"hist": lax.rem(me + k, n)}, device_id_type=pl.DeviceIdType.MESH
        )
    pl.semaphore_wait(barrier, n - 1)
    copies = []
    for k in range(1, n):
        peer = lax.rem(me + k, n)
        for src, dst, send, recv in ((stats, got_stats, send_b, recv_b), (parts, got, send_a, recv_a)):
            copy = pltpu.make_async_remote_copy(
                src_ref=src.at[peer],
                dst_ref=dst.at[k - 1],
                send_sem=send.at[k - 1],
                recv_sem=recv.at[k - 1],
                device_id={"hist": peer},
                device_id_type=pl.DeviceIdType.MESH,
            )
            copy.start()
            copies.append(copy)
    for copy in copies:
        copy.wait()
    logs = [stats[me]] + [got_stats[k] for k in range(n - 1)]
    highest = functools.reduce(jnp.maximum, logs)
    shares = [jnp.exp2(log - highest) for log in logs]
    inverse = 1.0 / functools.reduce(jnp.add, shares)
    embed = parts.shape[1]
    head = embed // H
    pieces = []
    for h in range(H):
        rows = slice(h * head, (h + 1) * head)
        mixed = parts[me, rows, :].astype(jnp.float32) * shares[0][h : h + 1, :]
        for k in range(n - 1):
            mixed += got[k, rows, :].astype(jnp.float32) * shares[k + 1][h : h + 1, :]
        pieces.append(mixed * inverse[h : h + 1, :])
    attended = jnp.concatenate(pieces, axis=0).astype(jnp.bfloat16)
    result[...] = lax.dot_general(
        attended, out_weight[3], (((0,), (0,)), ((), ())), preferred_element_type=jnp.float32
    ).astype(jnp.bfloat16)


def body(candidates, history, projections, lengths, selected):
    n = lax.axis_size("hist")
    ranks = lax.axis_size("dp")
    users, own_cands, embed = candidates.shape
    cands = n * own_cands
    line = n // 2
    own_rows = history.shape[1]
    blocks = own_rows // BLOCK
    first = (lax.axis_index("hist") * blocks).astype(jnp.int32)
    base = first.reshape(1)
    whole, weights, keys, values, flags = pl.pallas_call(
        functools.partial(gather_kernel, n, ranks),
        out_shape=[
            jax.ShapeDtypeStruct((users, cands, embed), jnp.bfloat16),
            jax.ShapeDtypeStruct((projections.shape[0], ranks * projections.shape[1], embed), jnp.bfloat16),
            jax.ShapeDtypeStruct((users, own_rows, embed), jnp.bfloat16),
            jax.ShapeDtypeStruct((users, embed, own_rows), jnp.bfloat16),
            jax.ShapeDtypeStruct((users, 128), jnp.int32),
        ],
        in_specs=[pl.BlockSpec(memory_space=pltpu.SMEM)]
        + [pl.BlockSpec(memory_space=pltpu.VMEM)] * 2
        + [pl.BlockSpec(memory_space=pl.ANY), pl.BlockSpec(memory_space=pltpu.VMEM)],
        out_specs=[pl.BlockSpec(memory_space=pltpu.VMEM)] * 2
        + [pl.BlockSpec(memory_space=pl.ANY)] * 2
        + [pl.BlockSpec(memory_space=pltpu.VMEM)],
        scratch_shapes=[
            pltpu.VMEM((users, own_rows, embed), jnp.bfloat16),
            pltpu.VMEM((users, own_rows, embed), jnp.bfloat16),
            pltpu.VMEM((users, embed, own_rows), jnp.bfloat16),
            pltpu.SemaphoreType.DMA((users + 1,)),
            pltpu.SemaphoreType.DMA((users,)),
            pltpu.SemaphoreType.DMA((2, users)),
            pltpu.SemaphoreType.DMA((line - 1, users)),
            pltpu.SemaphoreType.DMA((line - 1, users)),
            pltpu.SemaphoreType.DMA((line, users)),
            pltpu.SemaphoreType.DMA((line, users)),
            pltpu.SemaphoreType.DMA((ranks - 1,)),
            pltpu.SemaphoreType.DMA((ranks - 1,)),
        ],
        compiler_params=pltpu.CompilerParams(collective_id=1, has_side_effects=True),
        name="gather",
    )(lengths, candidates, projections, history, selected)
    wide = -(-users * own_cands // 128) * 128
    parts, stats = pl.pallas_call(
        functools.partial(attend_kernel, own_cands),
        grid_spec=pltpu.PrefetchScalarGridSpec(
            num_scalar_prefetch=3,
            grid=(users,),
            in_specs=[
                pl.BlockSpec((1, cands, embed), lambda u, *_: (u, 0, 0)),
                pl.BlockSpec((1, own_rows, embed), lambda u, *_: (u, 0, 0)),
                pl.BlockSpec((1, embed, own_rows), lambda u, *_: (u, 0, 0)),
                pl.BlockSpec((4, embed, embed), lambda u, *_: (0, 0, 0)),
            ],
            out_specs=[
                pl.BlockSpec((n, embed, wide), lambda u, *_: (0, 0, 0)),
                pl.BlockSpec((n, H, wide), lambda u, *_: (0, 0, 0)),
            ],
            scratch_shapes=[
                pltpu.VMEM((H, embed, cands), jnp.bfloat16),
                pltpu.VMEM((H, embed // H + 16, cands), jnp.float32),
                pltpu.VMEM((8, cands), jnp.float32),
                pltpu.VMEM((users, embed, cands), jnp.bfloat16),
                pltpu.VMEM((users, H, cands), jnp.float32),
                pltpu.SMEM((blocks + 8,), jnp.int32),
            ],
        ),
        out_shape=[
            jax.ShapeDtypeStruct((n, embed, wide), jnp.bfloat16),
            jax.ShapeDtypeStruct((n, H, wide), jnp.float32),
        ],
        name="attend",
    )(lengths, flags, base, whole, keys, values, weights)
    result = pl.pallas_call(
        functools.partial(combine_kernel, n),
        out_shape=jax.ShapeDtypeStruct((wide, embed), jnp.bfloat16),
        in_specs=[pl.BlockSpec(memory_space=pltpu.VMEM)] * 3,
        out_specs=pl.BlockSpec(memory_space=pltpu.VMEM),
        scratch_shapes=[
            pltpu.VMEM((n - 1, embed, wide), jnp.bfloat16),
            pltpu.VMEM((n - 1, H, wide), jnp.float32),
        ]
        + [pltpu.SemaphoreType.DMA((n - 1,))] * 4,
        compiler_params=pltpu.CompilerParams(collective_id=0, has_side_effects=True),
        name="combine",
    )(parts, stats, weights)
    return result[: users * own_cands].reshape(users, own_cands, embed)


def solution(mesh):
    placed = (
        P("dp", "hist", None),
        P("dp", "hist", None),
        P(None, "dp", None),
        P("dp"),
        P("dp", None),
    )
    return jax.shard_map(
        body, mesh=mesh, in_specs=placed, out_specs=P("dp", "hist", None), check_vma=False
    )
```
